32 devices in a mesh: dp: 32 (over z, y, x, core), tensor: 1.
Axes of the slice: x: 2, y: 2, z: 4, core: 2. Of those that a mesh axis runs over, the one named last changes fastest.
Arguments:
- latent_raw: bfloat16 [6144, 512], P('dp'), may hold values from -6 to 6
- norm_gain: float32 [512], replicated, may hold values from 0.5 to 1.5
- up_weight: bfloat16 [512, 4096], P(None, 'tensor'), may hold values from -0.25 to 0.25
- grad_kv: bfloat16 [6144, 4096], P('dp', 'tensor'), may hold values from -3 to 3
Outputs:
- latent_grad: bfloat16 [6144, 512], P('dp')
- gain_grad: float32 [512], replicated
- weight_grad: float32 [512, 4096], P('dp', 'tensor')
The draws below stay inside these ranges and needn't reach their ends.
All inputs are finite; a program needn't handle non-finite values.
Results may differ from the reference program's by a relative error of at most 0.0029.
Values may be sent and summed in bfloat16 or wider, within the bound.
A program may use at most 64 MiB of HBM per device.

```python
import jax
import jax.numpy as jnp
from jax import lax

KVL = 512
HEAD_DIM = 128
HEADS = 16
TOKENS = 6144


def strengthened(drawn, rng, source, target, blocks, factor):
    owner, partner = [(jnp.arange(drawn.shape[position]) // (drawn.shape[position] // blocks)).reshape([-1 if axis == position else 1 for axis in range(drawn.ndim)]) for position in (source, target)]
    chosen = jax.random.permutation(rng, blocks)[partner]
    strong = (owner == chosen) | (owner == (partner + blocks // 2) % blocks)
    return jnp.where(strong, factor * drawn, drawn)


def steps_of(rng, extent, shards, least, high):
    level = 1.0
    for position, parts in shards:
        draws = jax.random.uniform(jax.random.fold_in(jax.random.fold_in(rng, 6), position), (parts,), jnp.float32, least / len(shards), high / len(shards))
        level = level * jnp.repeat(jnp.exp(draws), extent[position] // parts).reshape((-1,) + (1,) * (len(extent) - 1 - position))
    return level


def noise(stream_key, shape, scale, bound, split=(), held_as=jnp.bfloat16):
    factor_of = steps_of(stream_key, shape, split, -0.22, 0.18) if split else 1.0
    entries = jax.random.normal(stream_key, shape, jnp.float32) * scale * factor_of
    return jnp.minimum(jnp.maximum(entries, -bound), bound).astype(held_as)


def bell_draw_with(stream_key, extent, spread, most, shards, heavy, dtype=jnp.bfloat16):
    array = spread * jax.random.normal(stream_key, extent, jnp.float32)
    if shards:
        array = array * steps_of(stream_key, extent, shards, -0.22, 0.18)
    return jnp.clip(strengthened(array, jax.random.fold_in(stream_key, 3), *heavy), -most, most).astype(dtype)


def setup_inputs(seed: int = 0) -> dict:
    arg_keys = jax.random.split(jax.random.key(seed), 5)
    return {
        "latent_raw": bell_draw_with(arg_keys[0], (TOKENS, KVL), 1.0, 6.0, ((0, 32),), (0, 1, 32, 2.75)),
        "norm_gain": jnp.clip(1.0 + 0.1 * jax.random.normal(arg_keys[1], (KVL,), jnp.float32), 0.5, 1.5),
        "up_weight": noise(arg_keys[2], (KVL, HEADS * 2 * HEAD_DIM), KVL ** -0.5, 0.25),
        "grad_kv": noise(arg_keys[3], (TOKENS, HEADS * 2 * HEAD_DIM), 0.5, 3.0, ((0, 32),)),
    }


epsilon = 1e-06

def reference(latent_raw, norm_gain, up_weight, grad_kv):
    latent_full = latent_raw.astype(jnp.float32)
    inverse = lax.rsqrt(lax.optimization_barrier(jnp.mean(latent_full * latent_full, axis=-1, keepdims=True)) + epsilon)
    scaled_rows = latent_full * inverse
    normed = (scaled_rows * norm_gain).astype(jnp.bfloat16)
    factor = float(TOKENS) ** (-0.5)
    grad_norm = lax.dot_general(grad_kv, up_weight, (((1,), (1,)), ((), ())), preferred_element_type=jnp.float32)
    gain_grad = lax.optimization_barrier(jnp.sum(grad_norm * scaled_rows, axis=0)) * factor
    upstream = grad_norm * norm_gain
    centred = upstream - scaled_rows * lax.optimization_barrier(jnp.mean(upstream * scaled_rows, axis=-1, keepdims=True))
    latent_grad = (inverse * centred).astype(jnp.bfloat16)
    weight_grad = lax.dot_general(normed, grad_kv, (((0,), (0,)), ((), ())), preferred_element_type=jnp.float32) * factor
    return (latent_grad, gain_grad, weight_grad)
```

```python
import functools

import jax
import jax.numpy as jnp
from jax import lax
from jax.experimental import pallas as pl
from jax.experimental.pallas import tpu as pltpu
from jax.sharding import PartitionSpec as P

epsilon = 1e-06
MESH = pl.DeviceIdType.MESH
FIRST_Z = (2, 4)
PAIRS = (2, 3, 2, 2, 2, 2)
GRANULES = 32
SEND, PASS, SPREAD, FINISH, NORM, GAIN = range(6)
NORMS = 3
ORDER = (
    (SEND, 0), (SEND, 2), (SEND, 3), (SEND, 1), (SEND, 4), (SEND, 5),
    (SEND, 6), (SEND, 7), (SEND, 8), (PASS, 2), (PASS, 3), (NORM, 0),
    (NORM, 1), (SEND, 9), (SEND, 10), (NORM, 2), (SEND, 11), (SEND, 12),
    (PASS, 4), (PASS, 5), (PASS, 0), (PASS, 6), (PASS, 7), (SPREAD, 2),
    (PASS, 8), (GAIN, 0), (SPREAD, 3), (PASS, 9), (SEND, 13), (PASS, 10),
    (PASS, 11), (PASS, 1), (SPREAD, 4), (PASS, 12), (FINISH, 2), (SPREAD, 6),
    (FINISH, 3), (SPREAD, 5), (SPREAD, 8), (FINISH, 0), (SPREAD, 7), (GAIN, 1),
    (SPREAD, 9), (PASS, 13), (FINISH, 4), (SPREAD, 11), (SPREAD, 10), (FINISH, 6),
    (FINISH, 1), (SPREAD, 12), (SPREAD, 13), (FINISH, 5), (FINISH, 8), (FINISH, 7),
    (FINISH, 9), (FINISH, 11), (GAIN, 2), (FINISH, 10), (FINISH, 12), (FINISH, 13),
)


def normalize(latent_raw):
    latent_full = latent_raw.astype(jnp.float32)
    inverse = lax.rsqrt(jnp.mean(latent_full * latent_full, axis=-1, keepdims=True) + epsilon)
    return (latent_full * inverse, inverse)


def norm_backward(grad_norm, scaled_rows, inverse, norm_gain):
    upstream = grad_norm * norm_gain
    centred = upstream - scaled_rows * jnp.mean(upstream * scaled_rows, axis=-1, keepdims=True)
    return (inverse * centred).astype(jnp.bfloat16)


def per_device(latent_raw, norm_gain, up_weight, grad_kv):
    scaled_rows, inverse = normalize(latent_raw)
    normed = (scaled_rows * norm_gain).astype(jnp.bfloat16)
    factor = float(latent_raw.shape[0] * lax.axis_size("dp")) ** (-0.5)
    partial_norm = lax.dot_general(
        grad_kv, up_weight, (((1,), (1,)), ((), ())), preferred_element_type=jnp.float32
    )
    grad_norm = lax.psum_scatter(partial_norm, "tensor", scatter_dimension=0, tiled=True)
    row_count = grad_norm.shape[0]
    offset = lax.axis_index("tensor") * row_count
    scaled_part = lax.dynamic_slice_in_dim(scaled_rows, offset, row_count, 0)
    inverse_part = lax.dynamic_slice_in_dim(inverse, offset, row_count, 0)
    gain_local = jnp.sum(grad_norm * scaled_part, axis=0)
    latent_part = norm_backward(grad_norm, scaled_part, inverse_part, norm_gain)
    latent_grad = lax.all_gather(latent_part, "tensor", axis=0, tiled=True)
    gain_grad = lax.psum(gain_local, ("dp", "tensor")) * factor
    weight_partial = lax.dot_general(
        normed, grad_kv, (((0,), (0,)), ((), ())), preferred_element_type=jnp.float32
    )
    weight_grad = lax.psum_scatter(weight_partial, "dp", scatter_dimension=0, tiled=True) * factor
    return (latent_grad, gain_grad, weight_grad)


def unit_list():
    units, start = [], 0
    for width in FIRST_Z:
        units.append(("z", start, width))
        start += width
    for width in PAIRS:
        for kind in ("x", "y"):
            units.append((kind, start, width))
            start += width
    return units


UNITS = unit_list()


def buffers(planes, kind, tokens, rows, width):
    bf16, f32 = jnp.bfloat16, jnp.float32
    shapes = [((tokens, width), bf16), ((tokens, width), bf16)]
    if kind == "z":
        shapes += [
            ((planes - 1, 4 * rows, width), bf16), ((planes - 1, 4 * rows, width), bf16),
            ((4 * rows, width), f32),
            ((3, rows, width), bf16), ((3, rows, width), bf16), ((rows, width), f32),
        ]
    else:
        half, quarter = 2 * planes * rows, planes * rows
        shapes += [
            ((half, width), bf16), ((half, width), bf16), ((half, width), f32),
            ((quarter, width), bf16), ((quarter, width), bf16), ((quarter, width), f32),
            ((planes - 1, rows, width), bf16), ((planes - 1, rows, width), bf16),
            ((rows, width), f32),
        ]
    return [pltpu.VMEM(shape, dtype) for shape, dtype in shapes]


def kernel(planes, factor, granule, *refs):
    refs = list(refs)

    def take(count):
        taken = refs[:count]
        del refs[:count]
        return taken

    latent_hbm, gain_hbm, weight_hbm, grad_hbm = take(4)
    latent_out, gain_out, weight_out = take(3)
    latent_ref, gain_ref, weight, turned, peer_turned, left = take(6)
    grad_norm, gain_send, gain_pair, gain_quad, gain_line = take(5)
    held = [take(8 if kind == "z" else 11) for kind, _, _ in UNITS]
    small_sem, local_sem, grad_sem, one_sem, two_sem, three_sem, gain_sem = take(7)

    rows = weight_out.shape[0]
    me = lax.axis_index("dp")
    core, x, y, z = me % 2, (me // 2) % 2, (me // 4) % 2, me // 8
    partner = me + 1 - 2 * core
    over_x = me + 2 - 4 * x
    over_y = me + 4 - 8 * y
    over_xy = over_x + 4 - 8 * y
    lines = [((z + step) % planes) * 8 + me % 8 for step in range(1, planes)]
    quad = [over_x, over_y, over_xy]
    peers = [partner] + quad + lines

    def columns(unit):
        _, start, width = UNITS[unit]
        return pl.ds(start * granule, width * granule)

    def send(source, target, send_sem, recv_sem, device):
        return pltpu.make_async_remote_copy(
            src_ref=source, dst_ref=target, send_sem=send_sem, recv_sem=recv_sem,
            device_id={"dp": device}, device_id_type=MESH,
        )

    small_loads = [
        pltpu.make_async_copy(latent_hbm, latent_ref, small_sem.at[0]),
        pltpu.make_async_copy(gain_hbm, gain_ref, small_sem.at[1]),
    ]
    for copy in small_loads:
        copy.start()
    firsts = [unit for stage, unit in ORDER if stage == SEND]
    loads = {}
    for unit in firsts:
        loads[unit] = pltpu.make_async_copy(
            grad_hbm.at[:, columns(unit)], held[unit][0], local_sem.at[unit]
        )
        loads[unit].start()

    barrier = pltpu.get_barrier_semaphore()
    for peer in peers:
        pl.semaphore_signal(barrier, inc=1, device_id={"dp": peer}, device_id_type=MESH)

    for copy in small_loads:
        copy.wait()
    scaled_rows, _ = normalize(latent_ref[...])
    normed = scaled_rows * gain_ref[...]
    flipped = normed.T.astype(jnp.bfloat16)
    flipped = flipped.reshape(planes * 4, 2, rows, flipped.shape[1])
    turned[0] = flipped[:, 0]
    turned[1] = flipped[:, 1]

    pl.semaphore_wait(barrier, len(peers))

    turned_copy = send(
        turned.at[1 - core], peer_turned, small_sem.at[0], small_sem.at[2], partner
    )
    turned_copy.start()
    grads = {}

    def share_grads(units):
        for unit in units:
            loads[unit].wait()
            grads[unit] = send(
                held[unit][0], held[unit][1], local_sem.at[unit], grad_sem.at[unit], partner
            )
            grads[unit].start()

    share_grads(firsts[:1])
    weight_load = pltpu.make_async_copy(weight_hbm, weight, small_sem.at[1])

    def block(step, away_y, away_x):
        to_y = (1 - y) if away_y else y
        to_x = (1 - x) if away_x else x
        return ((z + step) % planes) * 4 + to_y * 2 + to_x

    def arrange(kind, side, source):
        for step in range(planes):
            for first in range(2):
                for second in range(2):
                    if kind == "z":
                        place = step * 4 + first * 2 + second
                        left[0, side, place] = source(block(step, first, second))
                    else:
                        place = (first * 2 + second) * planes + step
                        if kind == "x":
                            index = block(step, second == 0, first == 0)
                        else:
                            index = block(step, first == 0, second == 0)
                        left[1 if kind == "x" else 2, side, place] = source(index)

    arrange("z", 0, lambda index: turned[core, index])
    share_grads(firsts[1:3])
    for kind in ("x", "y"):
        arrange(kind, 0, lambda index: turned[core, index])
    share_grads(firsts[3:])
    weight_load.start()
    turned_copy.wait_recv()
    arranged = set()

    half_rows = planes * 2 * rows
    quarter_rows = planes * rows
    local, ones, twos, threes = dict(grads), {}, {}, {}

    def partial_of(unit):
        kind = UNITS[unit][0]
        if kind not in arranged:
            arrange(kind, 1, lambda index: peer_turned[index])
            arranged.add(kind)
        which = ("z", "x", "y").index(kind)
        sides = [
            left[which, side].reshape(planes * 4 * rows, left.shape[-1]) for side in range(2)
        ]
        grads[unit].wait_recv()
        return jnp.dot(
            sides[0], held[unit][0][...], preferred_element_type=jnp.float32
        ) + jnp.dot(sides[1], held[unit][1][...], preferred_element_type=jnp.float32)

    def along_z(unit, source, target, recv_sem):
        for step, device in enumerate(lines):
            send(
                source.at[step], target.at[step], local_sem.at[unit], recv_sem, device
            ).start()
        return send(source, target, local_sem.at[unit], recv_sem, lines[0])

    def stage_send(unit):
        kind = UNITS[unit][0]
        partial = partial_of(unit)
        local[unit].wait_send()
        if kind == "z":
            outgoing, incoming, keep = held[unit][2:5]
            split = partial.reshape(planes, 4 * rows, partial.shape[1])
            outgoing[...] = split[1:].astype(jnp.bfloat16)
            keep[...] = split[0]
            local[unit] = ones[unit] = along_z(unit, outgoing, incoming, one_sem.at[unit])
        else:
            outgoing, incoming, keep = held[unit][2:5]
            outgoing[...] = partial[:half_rows].astype(jnp.bfloat16)
            keep[...] = partial[half_rows:]
            local[unit] = ones[unit] = send(
                outgoing, incoming, local_sem.at[unit], one_sem.at[unit],
                over_x if kind == "x" else over_y,
            )
            ones[unit].start()

    def stage_pass(unit):
        kind = UNITS[unit][0]
        ones[unit].wait_recv()
        local[unit].wait_send()
        incoming, keep = held[unit][3:5]
        total = keep[...]
        if kind == "z":
            for step in range(planes - 1):
                total = total + incoming[step].astype(jnp.float32)
            outgoing, landing, rest = held[unit][5:8]
            total = total.reshape(4, rows, total.shape[1])
            outgoing[...] = total[1:].astype(jnp.bfloat16)
            rest[...] = total[0]
            for slot, device in ((2, over_xy), (0, over_x), (1, over_y)):
                send(
                    outgoing.at[slot], landing.at[slot], local_sem.at[unit],
                    three_sem.at[unit], device,
                ).start()
            local[unit] = threes[unit] = send(
                outgoing, landing, local_sem.at[unit], three_sem.at[unit], over_x
            )
        else:
            total = total + incoming[...].astype(jnp.float32)
            outgoing, landing, rest = held[unit][5:8]
            outgoing[...] = total[:quarter_rows].astype(jnp.bfloat16)
            rest[...] = total[quarter_rows:]
            local[unit] = twos[unit] = send(
                outgoing, landing, local_sem.at[unit], two_sem.at[unit],
                over_y if kind == "x" else over_x,
            )
            twos[unit].start()

    def stage_spread(unit):
        twos[unit].wait_recv()
        local[unit].wait_send()
        landing, keep, outgoing, incoming, rest = held[unit][6:11]
        total = keep[...] + landing[...].astype(jnp.float32)
        total = total.reshape(planes, rows, total.shape[1])
        outgoing[...] = total[1:].astype(jnp.bfloat16)
        rest[...] = total[0]
        local[unit] = threes[unit] = along_z(unit, outgoing, incoming, three_sem.at[unit])

    def stage_finish(unit):
        threes[unit].wait_recv()
        incoming, keep = held[unit][-2:]
        total = keep[...]
        for index in range(incoming.shape[0]):
            total = total + incoming[index].astype(jnp.float32)
        weight_out[:, columns(unit)] = total * factor

    gains = {}

    def gain_start(stage, copies, whole):
        for copy in copies:
            copy.start()
        gains[stage] = whole

    def norm_piece(piece):
        if piece == 0:
            weight_load.wait()
        share = -(-len(firsts) // NORMS)
        total = None if piece == 0 else grad_norm[...]
        for unit in firsts[piece * share : (piece + 1) * share]:
            product = lax.dot_general(
                held[unit][0][...], weight[:, columns(unit)], (((1,), (1,)), ((), ())),
                preferred_element_type=jnp.float32,
            )
            total = product if total is None else total + product
        grad_norm[...] = total
        if piece == NORMS - 1:
            scaled, inverse = normalize(latent_ref[...])
            gain_send[0] = jnp.sum(total * scaled, axis=0, keepdims=True)
            copy = send(gain_send.at[0], gain_pair, gain_sem.at[0], gain_sem.at[1], partner)
            gain_start(0, [copy], copy)
            latent_out[...] = norm_backward(total, scaled, inverse, gain_ref[...])

    def gain_step(stage):
        gains[stage].wait_recv()
        gains[stage].wait_send()
        if stage == 0:
            gain_send[1] = gain_send[0] + gain_pair[...]
            copies = [
                send(gain_send.at[1], gain_quad.at[slot], gain_sem.at[0], gain_sem.at[2], device)
                for slot, device in enumerate(quad)
            ]
            whole = send(gain_quad, gain_quad, gain_sem.at[0], gain_sem.at[2], over_x)
            gain_start(1, copies, whole)
        elif stage == 1:
            value = (gain_send[1] + gain_quad[0]) + (gain_quad[1] + gain_quad[2])
            gain_send[2] = value
            gain_line[0] = value
            copies = [
                send(
                    gain_send.at[2], gain_line.at[step + 1],
                    gain_sem.at[0], gain_sem.at[3], device,
                )
                for step, device in enumerate(lines)
            ]
            landed = gain_line.at[pl.ds(1, planes - 1)]
            gain_start(2, copies, send(landed, landed, gain_sem.at[0], gain_sem.at[3], lines[0]))
        else:
            value = gain_line[z % planes]
            for plane in range(1, planes):
                value = value + gain_line[(z - plane + planes) % planes]
            gain_out[...] = value * factor

    stages = (stage_send, stage_pass, stage_spread, stage_finish, norm_piece, gain_step)
    for stage, unit in ORDER:
        stages[stage](unit)

    turned_copy.wait_send()
    for copy in local.values():
        copy.wait_send()


def place_kernel(first_in, second_in, third_in, first_out, second_out, third_out, sem):
    pairs = ((first_in, first_out), (second_in, second_out), (third_in, third_out))
    copies = [pltpu.make_async_copy(*pair, sem.at[at]) for at, pair in enumerate(pairs)]
    for copy in copies:
        copy.start()
    for copy in copies:
        copy.wait()


def place(*arrays):
    hbm = pl.BlockSpec(memory_space=pl.ANY)
    vmem = pl.BlockSpec(memory_space=pltpu.VMEM)
    return pl.pallas_call(
        place_kernel,
        out_shape=tuple(jax.ShapeDtypeStruct(a.shape, a.dtype) for a in arrays),
        in_specs=[vmem] * 3,
        out_specs=(hbm,) * 3,
        scratch_shapes=[pltpu.SemaphoreType.DMA((3,))],
        compiler_params=pltpu.CompilerParams(vmem_limit_bytes=8 * 1024 * 1024),
    )(*arrays)


def fused(latent_raw, norm_gain, up_weight, grad_kv):
    devices = lax.axis_size("dp")
    planes = devices // 8
    tokens, latent_width = latent_raw.shape
    total_columns = grad_kv.shape[1]
    granule = total_columns // GRANULES
    rows = latent_width // devices
    factor = float(tokens * devices) ** (-0.5)
    bf16, f32 = jnp.bfloat16, jnp.float32
    dma = pltpu.SemaphoreType.DMA
    vmem = pl.BlockSpec(memory_space=pltpu.VMEM)
    count = len(UNITS)
    held = []
    for kind, _, width in UNITS:
        held += buffers(planes, kind, tokens, rows, width * granule)
    latent_grad, gain_grad, weight_grad = pl.pallas_call(
        functools.partial(kernel, planes, factor, granule),
        out_shape=(
            pltpu.VMEM((tokens, latent_width), bf16),
            pltpu.VMEM((1, latent_width), f32),
            pltpu.VMEM((rows, total_columns), f32),
        ),
        in_specs=[pl.BlockSpec(memory_space=pltpu.HBM)] * 4,
        out_specs=(vmem, vmem, vmem),
        scratch_shapes=[
            pltpu.VMEM((tokens, latent_width), bf16),
            pltpu.VMEM((1, latent_width), f32),
            pltpu.VMEM((latent_width, total_columns), bf16),
            pltpu.VMEM((2, planes * 4, rows, tokens), bf16),
            pltpu.VMEM((planes * 4, rows, tokens), bf16),
            pltpu.VMEM((3, 2, planes * 4, rows, tokens), bf16),
            pltpu.VMEM((tokens, latent_width), f32),
            pltpu.VMEM((3, 1, latent_width), f32),
            pltpu.VMEM((1, latent_width), f32),
            pltpu.VMEM((3, 1, latent_width), f32),
            pltpu.VMEM((planes, 1, latent_width), f32),
            *held,
            dma((3,)), dma((count,)), dma((count,)), dma((count,)),
            dma((count,)), dma((count,)), dma((4,)),
        ],
        compiler_params=pltpu.CompilerParams(
            collective_id=0, has_side_effects=True, vmem_limit_bytes=67043328 - 512 * 1024
        ),
    )(latent_raw, norm_gain.reshape(1, latent_width), up_weight, grad_kv)
    latent_grad, gain_grad, weight_grad = place(latent_grad, gain_grad, weight_grad)
    return (latent_grad, gain_grad.reshape(latent_width), weight_grad)


def solution(mesh):
    devices = mesh.shape["dp"]
    covered = mesh.shape["tensor"] == 1 and devices % 8 == 0 and 16 <= devices <= 32
    in_specs = (P("dp", None), P(), P(None, "tensor"), P("dp", "tensor"))
    out_specs = (P("dp", None), P(), P("dp", "tensor"))
    return jax.shard_map(
        fused if covered else per_device,
        mesh=mesh, in_specs=in_specs, out_specs=out_specs, check_vma=False,
    )
```

```python
import functools

import jax
import jax.numpy as jnp
from jax import lax
from jax.experimental import pallas as pl
from jax.experimental.pallas import tpu as pltpu
from jax.sharding import PartitionSpec as P

epsilon = 1e-06
MESH = pl.DeviceIdType.MESH
FIRST_Z = (2, 2, 2, 2)
PAIRS = (2, 2, 4, 2, 2)
GRANULES = 32
SEND, PASS, SPREAD, FINISH, NORM, GAIN = range(6)
NORMS = 4
ORDER = (
    (SEND, 1), (SEND, 13), (SEND, 4), (SEND, 10), (SEND, 7), (SEND, 6),
    (SEND, 0), (SEND, 5), (PASS, 4), (PASS, 1), (SEND, 2), (PASS, 13),
    (PASS, 7), (PASS, 10), (PASS, 0), (SEND, 11), (SEND, 12), (NORM, 0),
    (SPREAD, 4), (SEND, 8), (PASS, 6), (SPREAD, 13), (PASS, 5), (SPREAD, 10),
    (SEND, 9), (SEND, 3), (PASS, 2), (NORM, 1), (NORM, 2), (SPREAD, 6),
    (PASS, 11), (SPREAD, 7), (PASS, 12), (NORM, 3), (PASS, 3), (PASS, 8),
    (GAIN, 0), (FINISH, 10), (PASS, 9), (SPREAD, 5), (SPREAD, 2), (SPREAD, 1),
    (FINISH, 13), (SPREAD, 12), (SPREAD, 11), (SPREAD, 0), (SPREAD, 9), (GAIN, 1),
    (SPREAD, 8), (SPREAD, 3), (FINISH, 7), (FINISH, 1), (FINISH, 0), (FINISH, 6),
    (FINISH, 11), (FINISH, 9), (FINISH, 3), (GAIN, 2), (FINISH, 4), (FINISH, 2),
    (FINISH, 5), (FINISH, 12), (FINISH, 8),
)


def normalize(latent_raw):
    latent_full = latent_raw.astype(jnp.float32)
    inverse = lax.rsqrt(jnp.mean(latent_full * latent_full, axis=-1, keepdims=True) + epsilon)
    return (latent_full * inverse, inverse)


def norm_backward(grad_norm, scaled_rows, inverse, norm_gain):
    upstream = grad_norm * norm_gain
    centred = upstream - scaled_rows * jnp.mean(upstream * scaled_rows, axis=-1, keepdims=True)
    return (inverse * centred).astype(jnp.bfloat16)


def per_device(latent_raw, norm_gain, up_weight, grad_kv):
    scaled_rows, inverse = normalize(latent_raw)
    normed = (scaled_rows * norm_gain).astype(jnp.bfloat16)
    factor = float(latent_raw.shape[0] * lax.axis_size("dp")) ** (-0.5)
    partial_norm = lax.dot_general(
        grad_kv, up_weight, (((1,), (1,)), ((), ())), preferred_element_type=jnp.float32
    )
    grad_norm = lax.psum_scatter(partial_norm, "tensor", scatter_dimension=0, tiled=True)
    row_count = grad_norm.shape[0]
    offset = lax.axis_index("tensor") * row_count
    scaled_part = lax.dynamic_slice_in_dim(scaled_rows, offset, row_count, 0)
    inverse_part = lax.dynamic_slice_in_dim(inverse, offset, row_count, 0)
    gain_local = jnp.sum(grad_norm * scaled_part, axis=0)
    latent_part = norm_backward(grad_norm, scaled_part, inverse_part, norm_gain)
    latent_grad = lax.all_gather(latent_part, "tensor", axis=0, tiled=True)
    gain_grad = lax.psum(gain_local, ("dp", "tensor")) * factor
    weight_partial = lax.dot_general(
        normed, grad_kv, (((0,), (0,)), ((), ())), preferred_element_type=jnp.float32
    )
    weight_grad = lax.psum_scatter(weight_partial, "dp", scatter_dimension=0, tiled=True) * factor
    return (latent_grad, gain_grad, weight_grad)


def unit_list():
    sizes = [("z", width) for width in FIRST_Z]
    sizes += [(kind, width) for width in PAIRS for kind in ("x", "y")]
    units, start = {}, 0
    for stage, unit in ORDER:
        if stage == SEND:
            kind, width = sizes[unit]
            units[unit] = (kind, start, width)
            start += width
    return [units[unit] for unit in range(len(sizes))]


def share_list():
    shares, start, end = [], 0, 0
    for stage, unit in ORDER:
        if stage == SEND:
            end += UNITS[unit][2]
            if len(shares) < 3 or end - start >= 6 or end == GRANULES:
                shares.append((start, end))
                start = end
    return shares


KINDS = ("z", "x", "y")
UNITS = unit_list()
SHARES = share_list()


def buffers(planes, kind, rows, width):
    bf16, f32 = jnp.bfloat16, jnp.float32
    if kind == "z":
        shapes = [
            ((3, 4 * rows, width), bf16), ((3, 4 * rows, width), bf16),
            ((4, 4 * rows, width), f32),
            ((2, 4 * rows, width), bf16), ((4 * rows, width), bf16),
            ((3, rows, width), bf16), ((3, rows, width), bf16), ((rows, width), f32),
        ]
    else:
        half, quarter = 2 * planes * rows, planes * rows
        shapes = [
            ((half, width), bf16), ((half, width), bf16), ((half, width), f32),
            ((quarter, width), bf16), ((quarter, width), bf16), ((quarter, width), f32),
            ((planes - 1, rows, width), bf16), ((planes - 1, rows, width), bf16),
            ((rows, width), f32),
        ]
    return [pltpu.VMEM(shape, dtype) for shape, dtype in shapes]


def kernel(planes, factor, granule, *refs):
    refs = list(refs)

    def take(count):
        taken = refs[:count]
        del refs[:count]
        return taken

    latent_hbm, gain_hbm, weight_hbm, grad_hbm = take(4)
    latent_out, gain_out, weight_out = take(3)
    latent_ref, gain_ref, own_grad, peer_grad, weight, turned, peer_turned, left = take(8)
    grad_norm, gain_send, gain_pair, gain_quad, gain_line = take(5)
    held = [take(8 if kind == "z" else 9) for kind, _, _ in UNITS]
    small_sem, load_sem, grad_sem, local_sem, one_sem, two_sem, three_sem, gain_sem = take(8)

    rows = weight_out.shape[0]
    me = lax.axis_index("dp")
    core, x, y, z = me % 2, (me // 2) % 2, (me // 4) % 2, me // 8
    partner = me + 1 - 2 * core
    over_x = me + 2 - 4 * x
    over_y = me + 4 - 8 * y
    over_xy = over_x + 4 - 8 * y
    lines = [((z + step) % planes) * 8 + me % 8 for step in range(1, planes)]
    side = z // 2
    inner = (z + side) % 2 == 1
    near, far_inner, far_end = z + 1 - 2 * (z % 2), 2 - side, 3 - 3 * side
    near_device, far_inner_device, far_end_device = [
        plane * 8 + me % 8 for plane in (near, far_inner, far_end)
    ]
    quad = [over_x, over_y, over_xy]
    peers = [partner] + quad + lines

    def columns(unit):
        _, start, width = UNITS[unit]
        return pl.ds(start * granule, width * granule)

    def send(source, target, send_sem, recv_sem, device):
        return pltpu.make_async_remote_copy(
            src_ref=source, dst_ref=target, send_sem=send_sem, recv_sem=recv_sem,
            device_id={"dp": device}, device_id_type=MESH,
        )

    small_loads = [
        pltpu.make_async_copy(latent_hbm, latent_ref, small_sem.at[0]),
        pltpu.make_async_copy(gain_hbm, gain_ref, small_sem.at[1]),
    ]
    for copy in small_loads:
        copy.start()
    loads = []
    for at, (start, end) in enumerate(SHARES):
        part = pl.ds(start * granule, (end - start) * granule)
        loads.append(
            pltpu.make_async_copy(grad_hbm.at[:, part], own_grad.at[:, part], load_sem.at[at])
        )

    def start_loads(chosen):
        for copy in chosen:
            copy.start()

    start_loads(loads[:3])

    barrier = pltpu.get_barrier_semaphore()
    for peer in peers:
        pl.semaphore_signal(barrier, inc=1, device_id={"dp": peer}, device_id_type=MESH)

    for copy in small_loads:
        copy.wait()
    start_loads(loads[3:])
    scaled_rows, _ = normalize(latent_ref[...])
    normed = scaled_rows * gain_ref[...]
    flipped = normed.T.astype(jnp.bfloat16)
    flipped = flipped.reshape(planes * 4, 2, rows, flipped.shape[1])
    turned[0] = flipped[:, 0]
    turned[1] = flipped[:, 1]

    pl.semaphore_wait(barrier, len(peers))

    turned_copy = send(
        turned.at[1 - core], peer_turned, small_sem.at[0], small_sem.at[2], partner
    )
    turned_copy.start()
    grads = []

    def share_grads(upto):
        for at in range(len(grads), upto):
            loads[at].wait()
            part = pl.ds(SHARES[at][0] * granule, (SHARES[at][1] - SHARES[at][0]) * granule)
            grads.append(
                send(
                    own_grad.at[:, part], peer_grad.at[:, part],
                    load_sem.at[at], grad_sem.at[at], partner,
                )
            )
            grads[at].start()

    share_grads(1)
    weight_load = pltpu.make_async_copy(weight_hbm, weight, small_sem.at[1])

    def block(plane, away_y, away_x):
        to_y = (1 - y) if away_y else y
        to_x = (1 - x) if away_x else x
        return plane * 4 + to_y * 2 + to_x

    by_role = (z, near, far_inner, far_end)
    by_step = [(z + step) % planes for step in range(planes)]

    def arrange(kind, side, source):
        for step in range(planes):
            for first in range(2):
                for second in range(2):
                    if kind == "z":
                        place = step * 4 + first * 2 + second
                        left[0, side, place] = source(block(by_role[step], first, second))
                    else:
                        place = (first * 2 + second) * planes + step
                        if kind == "x":
                            index = block(by_step[step], second == 0, first == 0)
                        else:
                            index = block(by_step[step], first == 0, second == 0)
                        left[KINDS.index(kind), side, place] = source(index)

    def left_of(unit, side):
        which = KINDS.index(UNITS[unit][0])
        return left[which, side].reshape(planes * 4 * rows, left.shape[-1])

    def own_part(unit):
        return jnp.dot(
            left_of(unit, 0), own_grad[:, columns(unit)], preferred_element_type=jnp.float32
        )

    firsts = [unit for stage, unit in ORDER if stage == SEND]
    kinds = []
    for stage, unit in ORDER:
        if stage == SEND and UNITS[unit][0] not in kinds:
            kinds.append(UNITS[unit][0])
    for count, kind in enumerate(kinds):
        arrange(kind, 0, lambda index: turned[core, index])
        if count == 0:
            early = own_part(firsts[0])
        share_grads(len(SHARES) if count == 2 else count + 2)
    weight_load.start()
    turned_copy.wait_recv()
    arrived = set()
    arranged = set()

    half_rows = planes * 2 * rows
    quarter_rows = planes * rows
    local, ones, twos, threes = {}, {}, {}, {}

    def partial_of(unit):
        kind, start, _ = UNITS[unit]
        for at, (first, end) in enumerate(SHARES):
            if first <= start < end and at not in arrived:
                grads[at].wait_recv()
                arrived.add(at)
        if kind not in arranged:
            arrange(kind, 1, lambda index: peer_turned[index])
            arranged.add(kind)
        own = early if unit == firsts[0] else own_part(unit)
        return own + jnp.dot(
            left_of(unit, 1), peer_grad[:, columns(unit)], preferred_element_type=jnp.float32
        )

    def along_z(unit, source, target, recv_sem):
        for step, device in enumerate(lines):
            send(
                source.at[step], target.at[step], local_sem.at[unit], recv_sem, device
            ).start()
        return send(source, target, local_sem.at[unit], recv_sem, lines[0])

    def to_near(unit):
        outgoing, incoming = held[unit][:2]
        sems = (local_sem.at[unit], one_sem.at[unit], near_device)
        return send(outgoing.at[0], incoming.at[0], *sems), send(outgoing, incoming, *sems)

    def to_far(unit):
        outgoing, incoming = held[unit][3:5]
        sems = (local_sem.at[unit], two_sem.at[unit])
        return (
            send(outgoing.at[1], incoming, *sems, far_end_device),
            send(outgoing.at[0], incoming, *sems, far_inner_device),
        )

    def stage_send(unit):
        kind = UNITS[unit][0]
        partial = partial_of(unit)
        if kind == "z":
            outgoing, incoming, keep = held[unit][:3]
            split = partial.reshape(planes, 4 * rows, partial.shape[1])
            outgoing[...] = split[1:].astype(jnp.bfloat16)
            keep[...] = split
            outward, inward = to_near(unit)

            @pl.when(inner)
            def _():
                outward.start()

            @pl.when(jnp.logical_not(inner))
            def _():
                inward.start()
        else:
            outgoing, incoming, keep = held[unit][:3]
            outgoing[...] = partial[:half_rows].astype(jnp.bfloat16)
            keep[...] = partial[half_rows:]
            local[unit] = ones[unit] = send(
                outgoing, incoming, local_sem.at[unit], one_sem.at[unit],
                over_x if kind == "x" else over_y,
            )
            ones[unit].start()

    def stage_pass(unit):
        kind = UNITS[unit][0]
        incoming, keep = held[unit][1:3]
        if kind == "z":
            outward, inward = to_near(unit)
            onward = held[unit][3]

            @pl.when(inner)
            def _():
                inward.wait_recv()
                outward.wait_send()
                onward[...] = (keep[2:4] + incoming[1:3].astype(jnp.float32)).astype(jnp.bfloat16)
                for copy in to_far(unit):
                    copy.start()

            @pl.when(jnp.logical_not(inner))
            def _():
                outward.wait_recv()
                inward.wait_send()
        else:
            ones[unit].wait_recv()
            local[unit].wait_send()
            total = keep[...]
            total = total + incoming[...].astype(jnp.float32)
            outgoing, landing, rest = held[unit][3:6]
            outgoing[...] = total[:quarter_rows].astype(jnp.bfloat16)
            rest[...] = total[quarter_rows:]
            local[unit] = twos[unit] = send(
                outgoing, landing, local_sem.at[unit], two_sem.at[unit],
                over_y if kind == "x" else over_x,
            )
            twos[unit].start()

    def stage_spread(unit):
        if UNITS[unit][0] == "z":
            copies = to_far(unit)
            copies[0].wait_recv()

            @pl.when(inner)
            def _():
                for copy in copies:
                    copy.wait_send()

            first, keep = held[unit][1:3]
            second, outgoing, landing, rest = held[unit][4:8]
            total = keep[0] + first[0].astype(jnp.float32) + second[...].astype(jnp.float32)
            total = total.reshape(4, rows, total.shape[1])
            outgoing[...] = total[1:].astype(jnp.bfloat16)
            rest[...] = total[0]
            for slot, device in ((2, over_xy), (0, over_x), (1, over_y)):
                send(
                    outgoing.at[slot], landing.at[slot], local_sem.at[unit],
                    three_sem.at[unit], device,
                ).start()
            local[unit] = threes[unit] = send(
                outgoing, landing, local_sem.at[unit], three_sem.at[unit], over_x
            )
            return
        twos[unit].wait_recv()
        local[unit].wait_send()
        landing, keep, outgoing, incoming, rest = held[unit][4:9]
        total = keep[...] + landing[...].astype(jnp.float32)
        total = total.reshape(planes, rows, total.shape[1])
        outgoing[...] = total[1:].astype(jnp.bfloat16)
        rest[...] = total[0]
        local[unit] = threes[unit] = along_z(unit, outgoing, incoming, three_sem.at[unit])

    def stage_finish(unit):
        threes[unit].wait_recv()
        incoming, keep = held[unit][-2:]
        total = keep[...]
        for index in range(incoming.shape[0]):
            total = total + incoming[index].astype(jnp.float32)
        weight_out[:, columns(unit)] = total * factor

    gains = {}

    def gain_start(stage, copies, whole):
        for copy in copies:
            copy.start()
        gains[stage] = whole

    def norm_piece(piece):
        if piece == 0:
            weight_load.wait()
        part = pl.ds(piece * GRANULES // NORMS * granule, GRANULES // NORMS * granule)
        total = lax.dot_general(
            own_grad[:, part], weight[:, part], (((1,), (1,)), ((), ())),
            preferred_element_type=jnp.float32,
        )
        if piece:
            total = grad_norm[...] + total
        grad_norm[...] = total
        if piece == NORMS - 1:
            scaled, inverse = normalize(latent_ref[...])
            gain_send[0] = jnp.sum(total * scaled, axis=0, keepdims=True)
            copy = send(gain_send.at[0], gain_pair, gain_sem.at[0], gain_sem.at[1], partner)
            gain_start(0, [copy], copy)
            latent_out[...] = norm_backward(total, scaled, inverse, gain_ref[...])

    def gain_step(stage):
        gains[stage].wait_recv()
        gains[stage].wait_send()
        if stage == 0:
            gain_send[1] = gain_send[0] + gain_pair[...]
            copies = [
                send(gain_send.at[1], gain_quad.at[slot], gain_sem.at[0], gain_sem.at[2], device)
                for slot, device in enumerate(quad)
            ]
            whole = send(gain_quad, gain_quad, gain_sem.at[0], gain_sem.at[2], over_x)
            gain_start(1, copies, whole)
        elif stage == 1:
            value = (gain_send[1] + gain_quad[0]) + (gain_quad[1] + gain_quad[2])
            gain_send[2] = value
            gain_line[0] = value
            copies = [
                send(
                    gain_send.at[2], gain_line.at[step + 1],
                    gain_sem.at[0], gain_sem.at[3], device,
                )
                for step, device in enumerate(lines)
            ]
            landed = gain_line.at[pl.ds(1, planes - 1)]
            gain_start(2, copies, send(landed, landed, gain_sem.at[0], gain_sem.at[3], lines[0]))
        else:
            value = gain_line[z % planes]
            for plane in range(1, planes):
                value = value + gain_line[(z - plane + planes) % planes]
            gain_out[...] = value * factor

    stages = (stage_send, stage_pass, stage_spread, stage_finish, norm_piece, gain_step)
    for stage, unit in ORDER:
        stages[stage](unit)

    turned_copy.wait_send()
    for copy in grads + list(local.values()):
        copy.wait_send()


def place_kernel(first_in, second_in, third_in, first_out, second_out, third_out, sem):
    pairs = ((first_in, first_out), (second_in, second_out), (third_in, third_out))
    copies = [pltpu.make_async_copy(*pair, sem.at[at]) for at, pair in enumerate(pairs)]
    for copy in copies:
        copy.start()
    for copy in copies:
        copy.wait()


def place(*arrays):
    hbm = pl.BlockSpec(memory_space=pl.ANY)
    vmem = pl.BlockSpec(memory_space=pltpu.VMEM)
    return pl.pallas_call(
        place_kernel,
        out_shape=tuple(jax.ShapeDtypeStruct(a.shape, a.dtype) for a in arrays),
        in_specs=[vmem] * 3,
        out_specs=(hbm,) * 3,
        scratch_shapes=[pltpu.SemaphoreType.DMA((3,))],
        compiler_params=pltpu.CompilerParams(vmem_limit_bytes=8 * 1024 * 1024),
    )(*arrays)


def fused(latent_raw, norm_gain, up_weight, grad_kv):
    devices = lax.axis_size("dp")
    planes = devices // 8
    tokens, latent_width = latent_raw.shape
    total_columns = grad_kv.shape[1]
    granule = total_columns // GRANULES
    rows = latent_width // devices
    factor = float(tokens * devices) ** (-0.5)
    bf16, f32 = jnp.bfloat16, jnp.float32
    dma = pltpu.SemaphoreType.DMA
    vmem = pl.BlockSpec(memory_space=pltpu.VMEM)
    count = len(UNITS)
    held = []
    for kind, _, width in UNITS:
        held += buffers(planes, kind, rows, width * granule)
    latent_grad, gain_grad, weight_grad = pl.pallas_call(
        functools.partial(kernel, planes, factor, granule),
        out_shape=(
            pltpu.VMEM((tokens, latent_width), bf16),
            pltpu.VMEM((1, latent_width), f32),
            pltpu.VMEM((rows, total_columns), f32),
        ),
        in_specs=[pl.BlockSpec(memory_space=pltpu.HBM)] * 4,
        out_specs=(vmem, vmem, vmem),
        scratch_shapes=[
            pltpu.VMEM((tokens, latent_width), bf16),
            pltpu.VMEM((1, latent_width), f32),
            pltpu.VMEM((tokens, total_columns), bf16),
            pltpu.VMEM((tokens, total_columns), bf16),
            pltpu.VMEM((latent_width, total_columns), bf16),
            pltpu.VMEM((2, planes * 4, rows, tokens), bf16),
            pltpu.VMEM((planes * 4, rows, tokens), bf16),
            pltpu.VMEM((3, 2, planes * 4, rows, tokens), bf16),
            pltpu.VMEM((tokens, latent_width), f32),
            pltpu.VMEM((3, 1, latent_width), f32),
            pltpu.VMEM((1, latent_width), f32),
            pltpu.VMEM((3, 1, latent_width), f32),
            pltpu.VMEM((planes, 1, latent_width), f32),
            *held,
            dma((3,)), dma((len(SHARES),)), dma((len(SHARES),)), dma((count,)),
            dma((count,)), dma((count,)), dma((count,)), dma((4,)),
        ],
        compiler_params=pltpu.CompilerParams(
            collective_id=0, has_side_effects=True, vmem_limit_bytes=67043328 - 512 * 1024
        ),
    )(latent_raw, norm_gain.reshape(1, latent_width), up_weight, grad_kv)
    latent_grad, gain_grad, weight_grad = place(latent_grad, gain_grad, weight_grad)
    return (latent_grad, gain_grad.reshape(latent_width), weight_grad)


def solution(mesh):
    devices = mesh.shape["dp"]
    covered = mesh.shape["tensor"] == 1 and devices == 32
    in_specs = (P("dp", None), P(), P(None, "tensor"), P("dp", "tensor"))
    out_specs = (P("dp", None), P(), P("dp", "tensor"))
    return jax.shard_map(
        fused if covered else per_device,
        mesh=mesh, in_specs=in_specs, out_specs=out_specs, check_vma=False,
    )
```
